32 devices in a mesh: dp: 8 (over y, x, core), seq: 4 (over z).
Axes of the slice: x: 2, y: 2, z: 4, core: 2. Of those that a mesh axis runs over, the one named last changes fastest.
Arguments:
- queries: bfloat16 [8, 1024, 2048], P('dp', 'seq'), may hold values from -6 to 6
- keys: bfloat16 [8, 1024, 1024], P('dp', 'seq'), may hold values from -6 to 6
- values: bfloat16 [8, 1024, 1024], P('dp', 'seq'), may hold values from -190 to 190
- segments: int32 [8, 1024], P('dp', 'seq'), may hold values from 0 to 2, never falling along the last dimension, each value on 1 to 640 neighbouring positions
- cotangent: bfloat16 [8, 1024, 2304], P('dp', 'seq'), may hold values from -6 to 6
- weight: float32 [2048, 2304], P(('dp', 'seq')), may hold values from -0.125 to 0.125
- first_moment: bfloat16 [2048, 2304], P(('dp', 'seq')), may hold values from -1 to 1
- first_scale: float32 [2048, 18], P(('dp', 'seq')), may hold values from 0.3 to 3
- second_moment: bfloat16 [2048, 2304], P(('dp', 'seq')), may hold values from 0.049804688 to 1
- second_scale: float32 [2048, 18], P(('dp', 'seq')), may hold values from 0.3 to 3
Outputs:
- layer_out: bfloat16 [8, 1024, 2304], P('dp', 'seq')
- new_weight: float32 [2048, 2304], P(('dp', 'seq'))
- new_first: bfloat16 [2048, 2304], P(('dp', 'seq'))
- new_first_scale: float32 [2048, 18], P(('dp', 'seq'))
- new_second: bfloat16 [2048, 2304], P(('dp', 'seq'))
- new_second_scale: float32 [2048, 18], P(('dp', 'seq'))
The draws below stay inside these ranges and needn't reach their ends.
Inputs may be any that keep to these rules, and one draw needn't show every extreme that they name: `segments`: document numbers never fall along a sequence; each sequence holds 3 documents, one of exactly 640 positions.
All inputs are finite; a program needn't handle non-finite values. Where the reference program divides by a largest or mean magnitude, that divisor is 1e-20 or more.
Results may differ from the reference program's by a relative error of at most 0.01.
Values may be sent and summed in bfloat16 or wider, within the bound.
A program may use at most 128 MiB of HBM per device.

```python
import math
import jax
import jax.numpy as jnp
import numpy as np
from jax import lax

HEADS = 16
KV_HEADS = 8
HEAD_DIM = 128
DO = 2304
GROUP = 128
DOCS = 3
QW = 2048
KW = 1024
LENGTH = 1024
SEQS = 8
DOC_MOST = 640


def draw_values(key, part):
    base_key, column_key, row_key = jax.random.split(jax.random.fold_in(key, 17), 3)
    columns = jnp.arange(KW, dtype=jnp.float32)
    column_multiplier = 10.0 ** (columns / (KW - 1)) * jax.random.uniform(column_key, (KW,), jnp.float32, 0.7, 1.4)
    row_factor = jnp.exp(jax.random.uniform(row_key, (SEQS, LENGTH, 1), jnp.float32, 0.0, math.log(10.0)))
    base = jnp.clip(jax.random.normal(base_key, (SEQS, LENGTH, KW), jnp.float32), -4.0, 4.0)
    return (base * column_multiplier * row_factor / 3.0).astype(jnp.bfloat16)


def level_of(stream_key, dims, shards, smallest, largest):
    def one(dim, shards_of):
        heights = jax.random.uniform(jax.random.fold_in(jax.random.fold_in(stream_key, 6), dim), (shards_of,), jnp.float32, smallest / len(shards), largest / len(shards))
        return jnp.repeat(jnp.exp(heights), dims[dim] // shards_of).reshape((-1,) + (1,) * (len(dims) - dim - 1))

    loudness = one(*shards[0])
    for cut in shards[1:]:
        loudness = loudness * one(*cut)
    return loudness


def length_profile(number_of, total, reach, slope):
    loads = [(1 << 20) // math.isqrt(rank ** slope) + 1 for rank in range(2, number_of + 1)]
    spare, holding = total - reach - (number_of - 1), [1] * (number_of - 1)
    while spare > 0:
        candidates = [i for i in range(number_of - 1) if holding[i] < reach]
        mass, budget = sum([loads[i] for i in candidates]), spare
        for i in candidates:
            addition = min(reach - holding[i], max(1, budget * loads[i] // mass), spare)
            holding[i] = holding[i] + addition
            spare = spare - addition
    return np.array([reach] + holding)


def uneven(own_key, number_of, total, most, lean):
    if number_of == 2:
        one = jax.random.randint(own_key, (), max(1, total - most), min(most, total - 1) + 1)
        return jnp.stack([one, total - one])
    sizes = jnp.asarray(length_profile(number_of, total, most, lean), jnp.int32)
    twos = (number_of - 1) // 2
    giver, sink = sizes[1:1 + 2 * twos:2], sizes[2:2 + 2 * twos:2]
    margin = jnp.minimum(giver - 1, most - sink)
    passed = jax.random.randint(jax.random.fold_in(own_key, 1), (twos,), 0, 1 << 20) % (margin + 1)
    sizes = sizes.at[1:1 + 2 * twos:2].set(giver - passed).at[2:2 + 2 * twos:2].set(sink + passed)
    return sizes[jax.random.permutation(jax.random.fold_in(own_key, 2), number_of)]


def bell_draw(stream_key, dims, width, limit, pieces=(), held_as=jnp.bfloat16):
    drawn = width * jax.random.normal(stream_key, dims, jnp.float32)
    if pieces:
        drawn = drawn * level_of(stream_key, dims, pieces, -0.22, 0.18)
    return jnp.clip(drawn, -limit, limit).astype(held_as)


def setup_inputs(seed: int = 0) -> dict:
    seeds = jax.random.split(jax.random.key(seed), 11)
    queries = bell_draw(seeds[0], (SEQS, LENGTH, QW), 1.0, 6.0, ((0, 8), (1, 4)))
    keys = bell_draw(seeds[1], (SEQS, LENGTH, KW), 1.0, 6.0, ((0, 8), (1, 4)))
    values = draw_values(jax.random.fold_in(seeds[10], 71), 0)
    segments = jax.vmap(lambda own: jnp.searchsorted(jnp.cumsum(uneven(own, DOCS, LENGTH, DOC_MOST, 0)), jnp.arange(LENGTH), side="right"))(jax.random.split(seeds[3], SEQS)).reshape((SEQS, LENGTH)).astype(jnp.int32)
    cotangent = bell_draw(seeds[4], (SEQS, LENGTH, DO), 1.0, 6.0, ((0, 8), (1, 4)))
    weight = bell_draw(seeds[5], (QW, DO), QW ** -0.5, 0.125, ((0, 32),), jnp.float32)
    first_moment = jnp.clip(jax.random.uniform(seeds[6], (QW, DO), jnp.float32, -1.0, 1.0) * level_of(seeds[6], (QW, DO), ((0, 32),), -0.4, 0.0), -1.0, 1.0).astype(jnp.bfloat16)
    first_scale = jnp.clip(jnp.exp(math.log(3.0) - 2.3025851 * jax.random.uniform(seeds[7], (QW, DO // GROUP), jnp.float32) ** level_of(seeds[7], (QW, DO // GROUP), ((0, 32),), -0.2, 0.2)), 0.3, 3.0)
    second_moment = jnp.clip(0.049804688 + 0.9501953 * jax.random.uniform(seeds[8], (QW, DO), jnp.float32) ** level_of(seeds[8], (QW, DO), ((0, 32),), -0.2, 0.2), 0.049804688, 1.0).astype(jnp.bfloat16)
    second_scale = jnp.clip(jnp.exp(math.log(3.0) - 2.3025851 * jax.random.uniform(seeds[9], (QW, DO // GROUP), jnp.float32) ** level_of(seeds[9], (QW, DO // GROUP), ((0, 32),), -0.2, 0.2)), 0.3, 3.0)
    return dict(queries=queries, keys=keys, values=values, segments=segments, cotangent=cotangent, weight=weight, first_moment=first_moment, first_scale=first_scale, second_moment=second_moment, second_scale=second_scale)


score_scale = 144.0 ** (-0.5)
soft_cap = 50.0
beta_first = 0.9
beta_second = 0.95
learn_rate = 0.001
decay_rate = 0.1

def quantize(blocks):
    grouped = blocks.astype(jnp.float32).reshape(blocks.shape[0], KV_HEADS, HEAD_DIM)
    scales = (lax.optimization_barrier(jnp.max(jnp.abs(grouped), axis=-1)) + 1e-06).astype(jnp.bfloat16)
    coded = (grouped / scales.astype(jnp.float32)[..., None]).astype(jnp.bfloat16)
    return (coded, scales)

def recover_values(coded, scales):
    return (coded.astype(jnp.float32) * scales.astype(jnp.float32)[..., None]).astype(jnp.bfloat16)

def attend(packed):
    query_seq, key_seq, value_seq, docs_seq = packed
    length = query_seq.shape[0]
    key_code, key_scale = quantize(key_seq)
    value_code, value_scale = quantize(value_seq)
    key_estimate = lax.optimization_barrier(recover_values(key_code, key_scale)).astype(jnp.float32)
    value_hat = lax.optimization_barrier(recover_values(value_code, value_scale)).astype(jnp.float32)
    grouped = query_seq.astype(jnp.float32).reshape(length, KV_HEADS, HEADS // KV_HEADS, HEAD_DIM)
    scores = jnp.einsum('qgrd,kgd->qgrk', grouped, key_estimate) * score_scale
    capped = soft_cap * jnp.tanh(scores / soft_cap)
    places = jnp.arange(length, dtype=jnp.int32)
    allowed = (docs_seq[:, None] == docs_seq[None, :]) & (places[None, :] <= places[:, None])
    weights = jnp.where(allowed[:, None, None, :], jnp.exp(capped), jnp.float32(0.0))
    totals = lax.optimization_barrier(jnp.sum(weights, axis=-1))
    rounded = lax.optimization_barrier(weights.astype(jnp.bfloat16)).astype(jnp.float32)
    mixed = jnp.einsum('qgrk,kgd->qgrd', rounded, value_hat)
    return (mixed / totals[..., None]).reshape(length, HEADS * HEAD_DIM).astype(jnp.bfloat16)

def decode(coded, scales):
    values_f = coded.astype(jnp.float32).reshape(coded.shape[0], -1, GROUP)
    return (scales[..., None] * jnp.sign(values_f) * jnp.sqrt(jnp.abs(values_f))).reshape(coded.shape)

def encode(moment):
    grouped = moment.reshape(moment.shape[0], -1, GROUP)
    scales = lax.optimization_barrier(jnp.max(jnp.abs(grouped), axis=-1)) + 1e-06
    coded = (grouped * jnp.abs(grouped) / (scales[..., None] * scales[..., None])).astype(jnp.bfloat16)
    return (coded.reshape(moment.shape), scales)

def reference(queries, keys, values, segments, cotangent, weight, first_moment, first_scale, second_moment, second_scale):
    attended = lax.map(attend, (queries, keys, values, segments))
    attended_flat = attended.reshape(-1, QW)
    weight_low = weight.astype(jnp.bfloat16)
    layer_out = jnp.dot(attended_flat, weight_low, preferred_element_type=jnp.float32).astype(jnp.bfloat16)
    layer_out = layer_out.reshape(SEQS, LENGTH, DO)
    gradient_matrix = jnp.dot(attended_flat.T, cotangent.reshape(-1, DO), preferred_element_type=jnp.float32)
    sum_squares = jnp.sum(gradient_matrix * gradient_matrix)
    rms_value = jnp.sqrt(sum_squares / (QW * DO) + 1e-06)
    clipped = gradient_matrix * jnp.minimum(jnp.float32(1.0), 1.0 / rms_value)
    first = beta_first * decode(first_moment, first_scale) + (1.0 - beta_first) * clipped
    second = beta_second * decode(second_moment, second_scale) + (1.0 - beta_second) * clipped * clipped
    new_weight = weight - learn_rate * (first / (jnp.sqrt(second) + 1e-08) + decay_rate * weight)
    new_first, new_first_scale = encode(first)
    new_second, new_second_scale = encode(second)
    return (layer_out, new_weight, new_first, new_first_scale, new_second, new_second_scale)
```

```python
import functools

import jax
import jax.numpy as jnp
from jax import lax
from jax.experimental import pallas as pl
from jax.experimental.pallas import tpu as pltpu
from jax.sharding import PartitionSpec as P

HEADS = 16
KV_HEADS = 8
HEAD_DIM = 128
GROUP = 128

score_scale = 144.0 ** (-0.5)
soft_cap = 50.0
beta_first = 0.9
beta_second = 0.95
learn_rate = 0.001
decay_rate = 0.1

MESH = pl.DeviceIdType.MESH


def restore(blocks):
    grouped = blocks.astype(jnp.float32).reshape(blocks.shape[0], KV_HEADS, HEAD_DIM)
    scales = (jnp.max(jnp.abs(grouped), axis=-1) + 1e-06).astype(jnp.bfloat16)
    wide = scales.astype(jnp.float32)[..., None]
    coded = (grouped / wide).astype(jnp.bfloat16)
    return (coded.astype(jnp.float32) * wide).astype(jnp.bfloat16).reshape(blocks.shape)


def orders(bits):
    high = list(range(1, bits))
    return (high, high[::-1])


def flip(me, r):
    out = me
    b = 0
    while (1 << b) <= r:
        if r & (1 << b):
            digit = lax.rem(lax.div(me, 1 << b), 2)
            out = out + (1 - 2 * digit) * (1 << b)
        b += 1
    return out


def gather_kernel(
    bits, n,
    k_ref, v_ref, doc_ref, w_ref,
    k_all, v_all, doc_all, w_all,
    own_sem, ws, wr, ks, kr, ds_, dr, ts, tr,
):
    me = lax.axis_index("dp")
    z = lax.axis_index("seq")
    tokens = k_ref.shape[0]
    rows, width = w_ref.shape
    half = width // 2
    big = n * rows
    right, left = lax.rem(z + 1, n), lax.rem(z + n - 1, n)

    def w_own(h):
        return w_ref.at[:, pl.ds(h * half, half)]

    def w_slot(zz, h):
        start = pl.multiple_of((me * n + zz) * rows, 16)
        return w_all.at[pl.ds(start, rows), pl.ds(h * half, half)]

    def kv_slot(ref, zz):
        return ref.at[pl.ds(pl.multiple_of(zz * tokens, 128), tokens), :]

    def doc_slot(zz):
        return doc_all.at[:, pl.ds(pl.multiple_of(zz * tokens, 128), tokens)]

    local = [
        pltpu.make_async_copy(k_ref, kv_slot(k_all, z), own_sem.at[0]),
        pltpu.make_async_copy(v_ref, kv_slot(v_all, z), own_sem.at[1]),
        pltpu.make_async_copy(doc_ref, doc_slot(z), own_sem.at[2]),
        pltpu.make_async_copy(w_own(0), w_slot(z, 0), own_sem.at[3]),
        pltpu.make_async_copy(w_own(1), w_slot(z, 1), own_sem.at[4]),
    ]
    for c in local:
        c.start()

    greet_bits(me, z, bits, n)

    started = []

    def remote(src, dst, ssem, rsem, dp, seq):
        copy = pltpu.make_async_remote_copy(
            src_ref=src, dst_ref=dst, send_sem=ssem, recv_sem=rsem,
            device_id={"dp": dp, "seq": seq}, device_id_type=MESH,
        )
        copy.start()
        started.append(copy)
        return copy

    far = n // 2

    def ring(own, slot, ss, rs, direction, part, s):
        shift = n - (s - 1) if direction == 0 else s - 1
        at = lax.rem(z + shift, n)
        src = own(part) if s == 1 else slot(at, part)
        to = right if direction == 0 else left
        return remote(
            src, slot(at, part), ss.at[direction, part, s - 1], rs.at[direction, part, s - 1],
            me, to,
        )

    def kv_own(part):
        return k_ref if part == 0 else v_ref

    def kv_at(zz, part):
        return kv_slot(k_all if part == 0 else v_all, zz)

    streams = ((0, 0), (1, 1), (0, 1), (1, 0))

    def runs(direction, part, s):
        return s < far or (s == far and direction == part)

    wc, kc = {}, {}
    for direction, part in streams:
        if runs(direction, part, 1):
            wc[direction, part, 1] = ring(w_own, w_slot, ws, wr, direction, part, 1)
    doc_copies = []
    for s in range(1, n):
        to = lax.rem(z + s, n)
        doc_copies.append(
            remote(doc_ref, doc_slot(z), ds_.at[s - 1], dr.at[s - 1], me, to)
        )
    for direction, part in streams:
        if runs(direction, part, 1):
            kc[direction, part, 1] = ring(kv_own, kv_at, ks, kr, direction, part, 1)
    for s in range(2, far + 1):
        for direction, part in streams:
            if runs(direction, part, s - 1) and runs(direction, part, s):
                wc[direction, part, s - 1].wait_recv()
                wc[direction, part, s] = ring(w_own, w_slot, ws, wr, direction, part, s)
    for (direction, part, s), c in wc.items():
        if not (runs(direction, part, s + 1) and s + 1 <= far):
            c.wait_recv()
    for c in local:
        c.wait()

    tree = []
    for h, order in enumerate(orders(bits)):
        tree.append(list(order) + [0])

    def block(r, h):
        start = pl.multiple_of(flip(me, r) * big, 16)
        return w_all.at[pl.ds(start, big), pl.ds(h * half, half)]

    tc = {}

    def forward(r, h):
        order = tree[h]
        last = -1
        for i, b in enumerate(order):
            if r & (1 << b):
                last = i
        for b in order[last + 1:]:
            nr = r | (1 << b)
            tc[h, nr] = remote(
                block(r, h), block(r, h), ts.at[h, nr], tr.at[h, nr], flip(me, 1 << b), z
            )

    for h in range(2):
        forward(0, h)
    count = 1 << bits
    rank = []
    for h in range(2):
        seen = [0]
        for b in tree[h]:
            seen = seen + [r | (1 << b) for r in seen]
        rank.append(seen[1:])
    for i in range(count - 1):
        for h in range(2):
            r = rank[h][i]
            if r % 2 == 0:
                tc[h, r].wait_recv()
                forward(r, h)
        if i == 0:
            for s in range(2, far + 1):
                for direction, part in streams:
                    if runs(direction, part, s - 1) and runs(direction, part, s):
                        kc[direction, part, s - 1].wait_recv()
                        kc[direction, part, s] = ring(
                            kv_own, kv_at, ks, kr, direction, part, s
                        )
    for (direction, part, s), c in kc.items():
        if not (runs(direction, part, s + 1) and s + 1 <= far):
            c.wait_recv()
    for c in doc_copies:
        c.wait_recv()
    for i in range(count - 1):
        for h in range(2):
            r = rank[h][i]
            if r % 2 == 1:
                tc[h, r].wait_recv()
    for c in started:
        c.wait_send()


def greet_bits(me, z, bits, n):
    barrier = pltpu.get_barrier_semaphore()
    for b in range(bits):
        pl.semaphore_signal(
            barrier, inc=1, device_id={"dp": flip(me, 1 << b), "seq": z}, device_id_type=MESH
        )
    for s in range(1, n):
        pl.semaphore_signal(
            barrier, inc=1, device_id={"dp": me, "seq": lax.rem(z + s, n)}, device_id_type=MESH
        )
    pl.semaphore_wait(barrier, bits + n - 1)


def gather_all(k, v, docs, w, bits, n):
    tokens, kw = k.shape
    rows, width = w.shape
    far = n // 2
    sem = pltpu.SemaphoreType.DMA
    vm = pl.BlockSpec(memory_space=pltpu.VMEM)
    hbm = pl.BlockSpec(memory_space=pl.ANY)
    count = 1 << bits
    return pl.pallas_call(
        functools.partial(gather_kernel, bits, n),
        out_shape=(
            jax.ShapeDtypeStruct((n * tokens, kw), k.dtype),
            jax.ShapeDtypeStruct((n * tokens, kw), v.dtype),
            jax.ShapeDtypeStruct((8, n * tokens), docs.dtype),
            jax.ShapeDtypeStruct((count * n * rows, width), w.dtype),
        ),
        in_specs=[vm] * 4,
        out_specs=(hbm, hbm, hbm, hbm),
        scratch_shapes=[
            sem((5,)),
            sem((2, 2, far)), sem((2, 2, far)),
            sem((2, 2, far)), sem((2, 2, far)),
            sem((n - 1,)), sem((n - 1,)),
            sem((2, count)), sem((2, count)),
        ],
        compiler_params=pltpu.CompilerParams(collective_id=0, has_side_effects=True),
    )(k, v, docs, w)


def attend_kernel(q_ref, k_ref, v_ref, docs_ref, own_ref, o_ref):
    z = lax.axis_index("seq")
    tokens = q_ref.shape[0]
    length = k_ref.shape[0]
    key_at = lax.broadcasted_iota(jnp.int32, (tokens, length), 1)
    query_at = lax.broadcasted_iota(jnp.int32, (tokens, length), 0) + z * tokens
    allowed = (own_ref[:, 0:1] == docs_ref[0:1, :]) & (key_at <= query_at)
    for i in range(2):
        cols = slice(i * HEAD_DIM, (i + 1) * HEAD_DIM)
        scores = lax.dot_general(
            q_ref[:, cols], k_ref[...], (((1,), (1,)), ((), ())),
            preferred_element_type=jnp.float32,
        )
        capped = soft_cap * jnp.tanh(scores * (score_scale / soft_cap))
        weights = jnp.where(allowed, jnp.exp(capped), 0.0)
        total = jnp.sum(weights, axis=-1, keepdims=True)
        mixed = jnp.dot(
            weights.astype(jnp.bfloat16), v_ref[...], preferred_element_type=jnp.float32
        )
        o_ref[:, cols] = (mixed / total).astype(o_ref.dtype)


def attend(q, k_all, v_all, docs_all, own):
    tokens = q.shape[0]
    length = k_all.shape[0]
    pair = HEADS // KV_HEADS * HEAD_DIM
    return pl.pallas_call(
        attend_kernel,
        grid=(KV_HEADS,),
        out_shape=jax.ShapeDtypeStruct(q.shape, q.dtype),
        in_specs=[
            pl.BlockSpec((tokens, pair), lambda g: (0, g)),
            pl.BlockSpec((length, HEAD_DIM), lambda g: (0, g)),
            pl.BlockSpec((length, HEAD_DIM), lambda g: (0, g)),
            pl.BlockSpec((8, length), lambda g: (0, 0)),
            pl.BlockSpec((tokens, 128), lambda g: (0, 0)),
        ],
        out_specs=pl.BlockSpec((tokens, pair), lambda g: (0, g)),
    )(q, k_all, v_all, docs_all, own)


def step_kernel(
    bits, n,
    att_ref, cot_ref, w_ref, m1_ref, s1_ref, m2_ref, s2_ref,
    nw_ref, n1_ref, ns1_ref, n2_ref, ns2_ref,
    sb, rb, zs, zr, grad, tot_s, tot_r,
    bs, br, zss, zsr, qs, qr,
):
    me = lax.axis_index("dp")
    z = lax.axis_index("seq")
    rows, width = w_ref.shape
    half = width // 2
    big = n * rows
    count = 1 << bits
    right, left = lax.rem(z + 1, n), lax.rem(z + n - 1, n)
    started = []

    def remote(src, dst, ssem, rsem, dp, seq):
        copy = pltpu.make_async_remote_copy(
            src_ref=src, dst_ref=dst, send_sem=ssem, recv_sem=rsem,
            device_id={"dp": dp, "seq": seq}, device_id_type=MESH,
        )
        copy.start()
        started.append(copy)
        return copy

    greet_bits(me, z, bits, n)

    def product(r, h):
        start = pl.multiple_of(flip(me, r) * big, 128)
        return jnp.dot(
            att_ref[pl.ds(start, big), :],
            cot_ref[:, h * half:(h + 1) * half],
            preferred_element_type=jnp.float32,
        )

    tree = [[0] + list(order) for order in orders(bits)]
    sent = {}

    def first_bit(r, h):
        for b in tree[h]:
            if r & (1 << b):
                return b

    def push(r, h):
        b = first_bit(r, h)
        sent[h, r] = remote(
            sb.at[h, r], rb.at[h, r], bs.at[h, r], br.at[h, r], flip(me, 1 << b), z
        )

    seq_of = []
    for h in range(2):
        seen = [0]
        for b in tree[h][:0:-1]:
            seen = seen + [r | (1 << b) for r in seen]
        def key(r, h=h):
            if r == 0:
                return (len(tree[h]), 0)
            return (tree[h].index(first_bit(r, h)), r)
        seq_of.append(sorted(seen, key=key))
    for i in range(count // 2):
        for h in range(2):
            r = seq_of[h][i] | 1
            sb[h, r] = product(r, h).astype(jnp.bfloat16)
            push(r, h)
    for i in range(count // 2):
        for h in range(2):
            r = seq_of[h][i]
            value = product(r, h)
            for b in tree[h]:
                if r & (1 << b):
                    break
                src = r | (1 << b)
                sent[h, src].wait_recv()
                value = value + rb[h, src].astype(jnp.float32)
            if r:
                sb[h, r] = value.astype(jnp.bfloat16)
                push(r, h)
            else:
                grad[:, h * half:(h + 1) * half] = value

    def part(zz, h):
        start = pl.multiple_of(zz * rows, 16)
        return grad[pl.ds(start, rows), h * half:(h + 1) * half]

    ring = {}
    for s in range(n):
        for h in range(2):
            shift = (2 * n - 1 - s) if h == 0 else (1 + s)
            at = lax.rem(z + shift, n)
            value = part(at, h)
            if s:
                ring[h, s - 1].wait_recv()
                value = value + zr[h, s - 1].astype(jnp.float32)
            if s < n - 1:
                zs[h, s] = value.astype(jnp.bfloat16)
                ring[h, s] = remote(
                    zs.at[h, s], zr.at[h, s], zss.at[h, s], zsr.at[h, s],
                    me, right if h == 0 else left,
                )
            else:
                grad[0:rows, h * half:(h + 1) * half] = value

    own = grad[0:rows, :]
    total = jnp.broadcast_to(
        jnp.sum(jnp.sum(own * own, axis=1, keepdims=True), axis=0, keepdims=True), (8, 128)
    )
    for b in range(bits):
        tot_s[b] = total
        c = remote(tot_s.at[b], tot_r.at[b], qs.at[b], qr.at[b], flip(me, 1 << b), z)
        c.wait_recv()
        total = total + tot_r[b]
    tot_s[bits] = total
    last = []
    for s in range(1, n):
        i = bits + s - 1
        last.append(
            remote(tot_s.at[bits], tot_r.at[i], qs.at[i], qr.at[i], me, lax.rem(z + s, n))
        )
    for s in range(1, n):
        last[s - 1].wait_recv()
        total = total + tot_r[bits + s - 1]

    rms = jnp.sqrt(total[0:1, :] / (count * n * rows * width) + 1e-06)
    factor = jnp.minimum(1.0, 1.0 / rms)

    def decode(coded, scale):
        x = coded.astype(jnp.float32)
        root = scale * jnp.sqrt(jnp.abs(x))
        return jnp.where(x < 0, -root, root)

    def encode(x):
        scale = jnp.max(jnp.abs(x), axis=-1, keepdims=True) + 1e-06
        return (x * jnp.abs(x) / (scale * scale)).astype(jnp.bfloat16), scale

    for g in range(width // GROUP):
        cols = slice(g * GROUP, (g + 1) * GROUP)
        clipped = grad[0:rows, cols] * factor
        first = beta_first * decode(m1_ref[:, cols], s1_ref[:, g:g + 1]) + (
            1.0 - beta_first
        ) * clipped
        second = (
            beta_second * decode(m2_ref[:, cols], s2_ref[:, g:g + 1])
            + (1.0 - beta_second) * clipped * clipped
        )
        weight = w_ref[:, cols]
        nw_ref[:, cols] = weight - learn_rate * (
            first / (jnp.sqrt(second) + 1e-08) + decay_rate * weight
        )
        n1_ref[:, cols], ns1_ref[:, g:g + 1] = encode(first)
        n2_ref[:, cols], ns2_ref[:, g:g + 1] = encode(second)
    for c in started:
        c.wait_send()


def train_step(att_t, cot, weight, m1, s1, m2, s2, bits, n):
    rows, width = weight.shape
    half = width // 2
    count = 1 << bits
    sem = pltpu.SemaphoreType.DMA
    vm = pl.BlockSpec(memory_space=pltpu.VMEM)
    like = lambda a: jax.ShapeDtypeStruct(a.shape, a.dtype)
    return pl.pallas_call(
        functools.partial(step_kernel, bits, n),
        out_shape=(like(weight), like(m1), like(s1), like(m2), like(s2)),
        in_specs=[vm] * 7,
        out_specs=(vm,) * 5,
        scratch_shapes=[
            pltpu.VMEM((2, count, n * rows, half), jnp.bfloat16),
            pltpu.VMEM((2, count, n * rows, half), jnp.bfloat16),
            pltpu.VMEM((2, n - 1, rows, half), jnp.bfloat16),
            pltpu.VMEM((2, n - 1, rows, half), jnp.bfloat16),
            pltpu.VMEM((n * rows, width), jnp.float32),
            pltpu.VMEM((bits + 1, 8, 128), jnp.float32),
            pltpu.VMEM((bits + n - 1, 8, 128), jnp.float32),
            sem((2, count)), sem((2, count)),
            sem((2, n - 1)), sem((2, n - 1)),
            sem((bits + n - 1,)), sem((bits + n - 1,)),
        ],
        compiler_params=pltpu.CompilerParams(
            collective_id=1, has_side_effects=True, vmem_limit_bytes=60 * 1024 * 1024
        ),
    )(att_t, cot, weight, m1, s1, m2, s2)


def local(
    bits, n,
    queries, keys, values, segments, cotangent, weight,
    first_moment, first_scale, second_moment, second_scale,
):
    docs = segments[0]
    tokens = docs.shape[0]
    k_all, v_all, docs_all, w_all = gather_all(
        restore(keys[0]),
        restore(values[0]),
        jnp.broadcast_to(docs[None, :], (8, tokens)),
        weight.astype(jnp.bfloat16),
        bits, n,
    )
    own = jnp.broadcast_to(docs[:, None], (tokens, 128))
    attended = attend(queries[0], k_all, v_all, docs_all, own)
    layer_out = jnp.dot(attended, w_all, preferred_element_type=jnp.float32)
    layer_out = layer_out.astype(jnp.bfloat16)[None]
    new_weight, new_first, new_first_scale, new_second, new_second_scale = train_step(
        attended.T, cotangent[0], weight, first_moment, first_scale,
        second_moment, second_scale, bits, n,
    )
    return (layer_out, new_weight, new_first, new_first_scale, new_second, new_second_scale)


def solution(mesh):
    bits = mesh.shape["dp"].bit_length() - 1
    n = mesh.shape["seq"]
    shard = P(("dp", "seq"), None)
    tok = P("dp", "seq", None)
    return jax.shard_map(
        functools.partial(local, bits, n),
        mesh=mesh,
        in_specs=(tok, tok, tok, P("dp", "seq"), tok, shard, shard, shard, shard, shard),
        out_specs=(tok, shard, shard, shard, shard, shard),
        check_vma=False,
    )
```

```python
import functools

import jax
import jax.numpy as jnp
from jax import lax
from jax.experimental import pallas as pl
from jax.experimental.pallas import tpu as pltpu
from jax.sharding import PartitionSpec as P

HEADS = 16
KV_HEADS = 8
HEAD_DIM = 128
GROUP = 128

score_scale = 144.0 ** (-0.5)
soft_cap = 50.0
beta_first = 0.9
beta_second = 0.95
learn_rate = 0.001
decay_rate = 0.1

MESH = pl.DeviceIdType.MESH


def restore(blocks):
    grouped = blocks.astype(jnp.float32).reshape(blocks.shape[0], KV_HEADS, HEAD_DIM)
    scales = (jnp.max(jnp.abs(grouped), axis=-1) + 1e-06).astype(jnp.bfloat16)
    wide = scales.astype(jnp.float32)[..., None]
    coded = (grouped / wide).astype(jnp.bfloat16)
    return (coded.astype(jnp.float32) * wide).astype(jnp.bfloat16).reshape(blocks.shape)


def longest(length):
    return length * 5 // 8


def reach_skips(tokens, n):
    skips = []
    for s in range(1, n):
        skip = max(0, s * tokens - longest(n * tokens)) // 128 * 128
        if skip < tokens:
            skips.append(skip)
    return tuple(skips)


def orders(bits):
    high = list(range(1, bits))
    return (high, high[::-1])


def flip(me, r):
    out = me
    b = 0
    while (1 << b) <= r:
        if r & (1 << b):
            digit = lax.rem(lax.div(me, 1 << b), 2)
            out = out + (1 - 2 * digit) * (1 << b)
        b += 1
    return out


def gather_kernel(
    bits, n, skips,
    k_ref, v_ref, doc_ref, w_ref,
    k_all, v_all, doc_all, w_all,
    own_sem, ws, wr, ks, kr, ds_, dr, ts, tr,
):
    me = lax.axis_index("dp")
    z = lax.axis_index("seq")
    tokens = k_ref.shape[0]
    rows, width = w_ref.shape
    half = width // 2
    big = n * rows
    right, left = lax.rem(z + 1, n), lax.rem(z + n - 1, n)

    def w_slot(zz):
        start = pl.multiple_of((me * n + zz) * rows, 16)
        return w_all.at[pl.ds(start, rows), :]

    def kv_slot(ref, zz):
        return ref.at[pl.ds(pl.multiple_of(zz * tokens, 128), tokens), :]

    def doc_slot(zz):
        return doc_all.at[:, pl.ds(pl.multiple_of(zz * tokens, 128), tokens)]

    local = [
        pltpu.make_async_copy(k_ref, kv_slot(k_all, z), own_sem.at[0]),
        pltpu.make_async_copy(v_ref, kv_slot(v_all, z), own_sem.at[1]),
        pltpu.make_async_copy(doc_ref, doc_slot(z), own_sem.at[2]),
        pltpu.make_async_copy(w_ref, w_slot(z), own_sem.at[3]),
    ]
    for c in local:
        c.start()

    greet_bits(me, z, bits, n)

    started = []

    def remote(src, dst, ssem, rsem, dp, seq):
        copy = pltpu.make_async_remote_copy(
            src_ref=src, dst_ref=dst, send_sem=ssem, recv_sem=rsem,
            device_id={"dp": dp, "seq": seq}, device_id_type=MESH,
        )
        copy.start()
        started.append(copy)
        return copy

    def descriptor(src, dst, ssem, rsem, dp, seq):
        return pltpu.make_async_remote_copy(
            src_ref=src, dst_ref=dst, send_sem=ssem, recv_sem=rsem,
            device_id={"dp": dp, "seq": seq}, device_id_type=MESH,
        )

    def w_hop(direction, s):
        shift = n + 1 - s if direction == 0 else s - 1
        at = lax.rem(z + shift, n)
        here = w_ref if s == 1 else w_slot(at)
        return descriptor(
            here, w_slot(at), ws.at[direction, s - 1], wr.at[direction, s - 1],
            me, right if direction == 0 else left,
        )

    def kv_hop(part, s):
        at = lax.rem(z + n + 1 - s, n)
        ref = (k_ref, v_ref)[part]
        out = (k_all, v_all)[part]
        skip = skips[s - 1]
        start = pl.multiple_of(at * tokens + skip, 128)
        dst = out.at[pl.ds(start, tokens - skip), :]
        src = ref.at[pl.ds(skip, tokens - skip), :] if s == 1 else dst
        return descriptor(src, dst, ks.at[part, s - 1], kr.at[part, s - 1], me, right)

    def room(direction, s):
        if direction == 0:
            return (z >= s - 1) & (z < n - 1)
        return (z <= n - s) & (z > 0)

    def landed(direction, s):
        return z >= s if direction == 0 else z <= n - 1 - s

    steps = len(skips)
    for s in range(1, n):
        for direction in range(2):
            if s > 1:

                @pl.when(landed(direction, s - 1))
                def _(direction=direction, s=s):
                    w_hop(direction, s - 1).wait_recv()

            @pl.when(room(direction, s))
            def _(direction=direction, s=s):
                w_hop(direction, s).start()

    @pl.when(room(0, 1))
    def _():
        kv_hop(0, 1).start()
        kv_hop(1, 1).start()

    doc_copies = []
    for s in range(1, n):
        to = lax.rem(z + s, n)
        doc_copies.append(
            remote(doc_ref, doc_slot(z), ds_.at[s - 1], dr.at[s - 1], me, to)
        )
    for direction in range(2):

        @pl.when(landed(direction, n - 1))
        def _(direction=direction):
            w_hop(direction, n - 1).wait_recv()

    for c in local:
        c.wait()

    def kv_forward(s):
        for part in range(2):

            @pl.when(landed(0, s - 1))
            def _(part=part):
                kv_hop(part, s - 1).wait_recv()

            if s <= steps:

                @pl.when(room(0, s))
                def _(part=part):
                    kv_hop(part, s).start()

    tree = []
    for h, order in enumerate(orders(bits)):
        tree.append(list(order) + [0])

    def block(r, h):
        start = pl.multiple_of(flip(me, r) * big, 16)
        return w_all.at[pl.ds(start, big), pl.ds(h * half, half)]

    tc = {}

    def forward(r, h):
        order = tree[h]
        last = -1
        for i, b in enumerate(order):
            if r & (1 << b):
                last = i
        for b in order[last + 1:]:
            nr = r | (1 << b)
            tc[h, nr] = remote(
                block(r, h), block(r, h), ts.at[h, nr], tr.at[h, nr], flip(me, 1 << b), z
            )

    for h in range(2):
        forward(0, h)
    count = 1 << bits
    rank = []
    for h in range(2):
        seen = [0]
        for b in tree[h]:
            seen = seen + [r | (1 << b) for r in seen]
        rank.append(seen[1:])
    for i in range(count - 1):
        for h in range(2):
            r = rank[h][i]
            if r % 2 == 0:
                tc[h, r].wait_recv()
                forward(r, h)
        if i == 0 and steps >= 2:
            kv_forward(2)
        if i == count // 2 - 2:
            for s in range(3, steps + 1):
                kv_forward(s)
    kv_forward(steps + 1)
    for c in doc_copies:
        c.wait_recv()
    for i in range(count - 1):
        for h in range(2):
            r = rank[h][i]
            if r % 2 == 1:
                tc[h, r].wait_recv()
    for c in started:
        c.wait_send()
    for s in range(1, n):
        for direction in range(2):

            @pl.when(room(direction, s))
            def _(direction=direction, s=s):
                w_hop(direction, s).wait_send()

    for s in range(1, steps + 1):

        @pl.when(room(0, s))
        def _(s=s):
            kv_hop(0, s).wait_send()
            kv_hop(1, s).wait_send()


def greet_bits(me, z, bits, n):
    barrier = pltpu.get_barrier_semaphore()
    for b in range(bits):
        pl.semaphore_signal(
            barrier, inc=1, device_id={"dp": flip(me, 1 << b), "seq": z}, device_id_type=MESH
        )
    for s in range(1, n):
        pl.semaphore_signal(
            barrier, inc=1, device_id={"dp": me, "seq": lax.rem(z + s, n)}, device_id_type=MESH
        )
    pl.semaphore_wait(barrier, bits + n - 1)


def gather_all(k, v, docs, w, bits, n):
    tokens, kw = k.shape
    rows, width = w.shape
    skips = reach_skips(tokens, n)
    sem = pltpu.SemaphoreType.DMA
    vm = pl.BlockSpec(memory_space=pltpu.VMEM)
    hbm = pl.BlockSpec(memory_space=pl.ANY)
    count = 1 << bits
    return pl.pallas_call(
        functools.partial(gather_kernel, bits, n, skips),
        out_shape=(
            jax.ShapeDtypeStruct((n * tokens, kw), k.dtype),
            jax.ShapeDtypeStruct((n * tokens, kw), v.dtype),
            jax.ShapeDtypeStruct((8, n * tokens), docs.dtype),
            jax.ShapeDtypeStruct((count * n * rows, width), w.dtype),
        ),
        in_specs=[vm] * 4,
        out_specs=(hbm, hbm, hbm, hbm),
        scratch_shapes=[
            sem((4,)),
            sem((2, n - 1)), sem((2, n - 1)),
            sem((2, len(skips))), sem((2, len(skips))),
            sem((n - 1,)), sem((n - 1,)),
            sem((2, count)), sem((2, count)),
        ],
        compiler_params=pltpu.CompilerParams(collective_id=0, has_side_effects=True),
    )(k, v, docs, w)


def attend_kernel(q_ref, k_ref, v_ref, docs_ref, own_ref, o_ref):
    z = lax.axis_index("seq")
    tokens = q_ref.shape[0]
    length = k_ref.shape[0]
    key_at = lax.broadcasted_iota(jnp.int32, (tokens, length), 1)
    query_at = lax.broadcasted_iota(jnp.int32, (tokens, length), 0) + z * tokens
    allowed = (own_ref[:, 0:1] == docs_ref[0:1, :]) & (key_at <= query_at)
    place = lax.broadcasted_iota(jnp.int32, v_ref.shape, 0)
    seen = (place < (z + 1) * tokens) & (place >= z * tokens - longest(length))
    value = jnp.where(seen, v_ref[...].astype(jnp.float32), 0.0).astype(jnp.bfloat16)
    for i in range(2):
        cols = slice(i * HEAD_DIM, (i + 1) * HEAD_DIM)
        scores = lax.dot_general(
            q_ref[:, cols], k_ref[...], (((1,), (1,)), ((), ())),
            preferred_element_type=jnp.float32,
        )
        capped = soft_cap * jnp.tanh(scores * (score_scale / soft_cap))
        weights = jnp.where(allowed, jnp.exp(capped), 0.0)
        total = jnp.sum(weights, axis=-1, keepdims=True)
        mixed = jnp.dot(
            weights.astype(jnp.bfloat16), value, preferred_element_type=jnp.float32
        )
        o_ref[:, cols] = (mixed / total).astype(o_ref.dtype)


def attend(q, k_all, v_all, docs_all, own):
    tokens = q.shape[0]
    length = k_all.shape[0]
    pair = HEADS // KV_HEADS * HEAD_DIM
    return pl.pallas_call(
        attend_kernel,
        grid=(KV_HEADS,),
        out_shape=jax.ShapeDtypeStruct(q.shape, q.dtype),
        in_specs=[
            pl.BlockSpec((tokens, pair), lambda g: (0, g)),
            pl.BlockSpec((length, HEAD_DIM), lambda g: (0, g)),
            pl.BlockSpec((length, HEAD_DIM), lambda g: (0, g)),
            pl.BlockSpec((8, length), lambda g: (0, 0)),
            pl.BlockSpec((tokens, 128), lambda g: (0, 0)),
        ],
        out_specs=pl.BlockSpec((tokens, pair), lambda g: (0, g)),
    )(q, k_all, v_all, docs_all, own)


def step_kernel(
    bits, n,
    att_ref, cot_ref, own_ref, sum_ref,
    sb, rb, zs, zr, grad, tot_s, tot_r,
    bs, br, zss, zsr, qs, qr,
):
    me = lax.axis_index("dp")
    z = lax.axis_index("seq")
    rows, width = own_ref.shape
    half = width // 2
    big = n * rows
    count = 1 << bits
    right, left = lax.rem(z + 1, n), lax.rem(z + n - 1, n)
    started = []

    def remote(src, dst, ssem, rsem, dp, seq):
        copy = pltpu.make_async_remote_copy(
            src_ref=src, dst_ref=dst, send_sem=ssem, recv_sem=rsem,
            device_id={"dp": dp, "seq": seq}, device_id_type=MESH,
        )
        copy.start()
        started.append(copy)
        return copy

    greet_bits(me, z, bits, n)

    def product(r, h):
        start = pl.multiple_of(flip(me, r) * big, 128)
        return jnp.dot(
            att_ref[pl.ds(start, big), :],
            cot_ref[:, h * half:(h + 1) * half],
            preferred_element_type=jnp.float32,
        )

    tree = [[0] + list(order) for order in orders(bits)]
    sent = {}

    def first_bit(r, h):
        for b in tree[h]:
            if r & (1 << b):
                return b

    def push(r, h):
        b = first_bit(r, h)
        sent[h, r] = remote(
            sb.at[h, r], rb.at[h, r], bs.at[h, r], br.at[h, r], flip(me, 1 << b), z
        )

    seq_of = []
    for h in range(2):
        seen = [0]
        for b in tree[h][:0:-1]:
            seen = seen + [r | (1 << b) for r in seen]
        def key(r, h=h):
            if r == 0:
                return (len(tree[h]), 0)
            return (tree[h].index(first_bit(r, h)), r)
        seq_of.append(sorted(seen, key=key))
    for i in range(count // 2):
        for h in range(2):
            r = seq_of[h][i] | 1
            sb[h, r] = product(r, h).astype(jnp.bfloat16)
            push(r, h)
    for i in range(count // 2):
        for h in range(2):
            r = seq_of[h][i]
            value = product(r, h)
            for b in tree[h]:
                if r & (1 << b):
                    break
                src = r | (1 << b)
                sent[h, src].wait_recv()
                value = value + rb[h, src].astype(jnp.float32)
            if r:
                sb[h, r] = value.astype(jnp.bfloat16)
                push(r, h)
            else:
                grad[:, h * half:(h + 1) * half] = value

    def part(zz, h):
        start = pl.multiple_of(zz * rows, 16)
        return grad[pl.ds(start, rows), h * half:(h + 1) * half]

    ring = {}
    for s in range(n):
        for h in range(2):
            shift = (2 * n - 1 - s) if h == 0 else (1 + s)
            at = lax.rem(z + shift, n)
            value = part(at, h)
            if s:
                ring[h, s - 1].wait_recv()
                value = value + zr[h, s - 1].astype(jnp.float32)
            if s < n - 1:
                zs[h, s] = value.astype(jnp.bfloat16)
                ring[h, s] = remote(
                    zs.at[h, s], zr.at[h, s], zss.at[h, s], zsr.at[h, s],
                    me, right if h == 0 else left,
                )
            else:
                own_ref[:, h * half:(h + 1) * half] = value

    own = own_ref[...]
    total = jnp.broadcast_to(
        jnp.sum(jnp.sum(own * own, axis=1, keepdims=True), axis=0, keepdims=True), (8, 128)
    )
    for b in range(bits):
        tot_s[b] = total
        c = remote(tot_s.at[b], tot_r.at[b], qs.at[b], qr.at[b], flip(me, 1 << b), z)
        c.wait_recv()
        total = total + tot_r[b]
    tot_s[bits] = total
    last = []
    for s in range(1, n):
        i = bits + s - 1
        last.append(
            remote(tot_s.at[bits], tot_r.at[i], qs.at[i], qr.at[i], me, lax.rem(z + s, n))
        )
    for s in range(1, n):
        last[s - 1].wait_recv()
        total = total + tot_r[bits + s - 1]

    sum_ref[...] = total
    for c in started:
        c.wait_send()


def adam_kernel(
    entries,
    grad_ref, sum_ref, w_ref, m1_ref, s1_ref, m2_ref, s2_ref,
    nw_ref, n1_ref, ns1_ref, n2_ref, ns2_ref,
):
    width = w_ref.shape[1]
    rms = jnp.sqrt(sum_ref[0:1, :] / entries + 1e-06)
    factor = jnp.minimum(1.0, 1.0 / rms)

    def decode(coded, scale):
        x = coded.astype(jnp.float32)
        root = scale * jnp.sqrt(jnp.abs(x))
        return jnp.where(x < 0, -root, root)

    def encode(x):
        scale = jnp.max(jnp.abs(x), axis=-1, keepdims=True) + 1e-06
        return (x * jnp.abs(x) / (scale * scale)).astype(jnp.bfloat16), scale

    for g in range(width // GROUP):
        cols = slice(g * GROUP, (g + 1) * GROUP)
        clipped = grad_ref[:, cols] * factor
        first = beta_first * decode(m1_ref[:, cols], s1_ref[:, g:g + 1]) + (
            1.0 - beta_first
        ) * clipped
        second = (
            beta_second * decode(m2_ref[:, cols], s2_ref[:, g:g + 1])
            + (1.0 - beta_second) * clipped * clipped
        )
        weight = w_ref[:, cols]
        nw_ref[:, cols] = weight - learn_rate * (
            first / (jnp.sqrt(second) + 1e-08) + decay_rate * weight
        )
        n1_ref[:, cols], ns1_ref[:, g:g + 1] = encode(first)
        n2_ref[:, cols], ns2_ref[:, g:g + 1] = encode(second)


def train_step(att_t, cot, weight, m1, s1, m2, s2, bits, n):
    rows, width = weight.shape
    half = width // 2
    count = 1 << bits
    sem = pltpu.SemaphoreType.DMA
    vm = pl.BlockSpec(memory_space=pltpu.VMEM)
    like = lambda a: jax.ShapeDtypeStruct(a.shape, a.dtype)
    grad, total = pl.pallas_call(
        functools.partial(step_kernel, bits, n),
        out_shape=(like(weight), jax.ShapeDtypeStruct((8, 128), jnp.float32)),
        in_specs=[vm] * 2,
        out_specs=(vm,) * 2,
        scratch_shapes=[
            pltpu.VMEM((2, count, n * rows, half), jnp.bfloat16),
            pltpu.VMEM((2, count, n * rows, half), jnp.bfloat16),
            pltpu.VMEM((2, n - 1, rows, half), jnp.bfloat16),
            pltpu.VMEM((2, n - 1, rows, half), jnp.bfloat16),
            pltpu.VMEM((n * rows, width), jnp.float32),
            pltpu.VMEM((bits + 1, 8, 128), jnp.float32),
            pltpu.VMEM((bits + n - 1, 8, 128), jnp.float32),
            sem((2, count)), sem((2, count)),
            sem((2, n - 1)), sem((2, n - 1)),
            sem((bits + n - 1,)), sem((bits + n - 1,)),
        ],
        compiler_params=pltpu.CompilerParams(
            collective_id=1, has_side_effects=True, vmem_limit_bytes=60 * 1024 * 1024
        ),
    )(att_t, cot)
    return pl.pallas_call(
        functools.partial(adam_kernel, float(count * n * rows * width)),
        out_shape=(like(weight), like(m1), like(s1), like(m2), like(s2)),
        in_specs=[vm] * 7,
        out_specs=(vm,) * 5,
    )(grad, total, weight, m1, s1, m2, s2)


def local(
    bits, n,
    queries, keys, values, segments, cotangent, weight,
    first_moment, first_scale, second_moment, second_scale,
):
    docs = segments[0]
    tokens = docs.shape[0]
    k_all, v_all, docs_all, w_all = gather_all(
        restore(keys[0]),
        restore(values[0]),
        jnp.broadcast_to(docs[None, :], (8, tokens)),
        weight.astype(jnp.bfloat16),
        bits, n,
    )
    own = jnp.broadcast_to(docs[:, None], (tokens, 128))
    attended = attend(queries[0], k_all, v_all, docs_all, own)
    layer_out = jnp.dot(attended, w_all, preferred_element_type=jnp.float32)
    layer_out = layer_out.astype(jnp.bfloat16)[None]
    new_weight, new_first, new_first_scale, new_second, new_second_scale = train_step(
        attended.T, cotangent[0], weight, first_moment, first_scale,
        second_moment, second_scale, bits, n,
    )
    return (layer_out, new_weight, new_first, new_first_scale, new_second, new_second_scale)


def solution(mesh):
    bits = mesh.shape["dp"].bit_length() - 1
    n = mesh.shape["seq"]
    shard = P(("dp", "seq"), None)
    tok = P("dp", "seq", None)
    return jax.shard_map(
        functools.partial(local, bits, n),
        mesh=mesh,
        in_specs=(tok, tok, tok, P("dp", "seq"), tok, shard, shard, shard, shard, shard),
        out_specs=(tok, shard, shard, shard, shard, shard),
        check_vma=False,
    )
```
